32 devices in a mesh: edp: 2 (over y), ep: 16 (over z, x, core).
Axes of the slice: x: 2, y: 2, z: 4, core: 2. Of those that a mesh axis runs over, the one named last changes fastest.
Arguments:
- tokens: bfloat16 [4096, 2048], P(('edp', 'ep')), may hold values from -6 to 6
- routes: int32 [4096, 8], P(('edp', 'ep')), may hold values from 0 to 15, all different within a row; in each aligned block of 128 rows (0 to 127, 128 to 255, ...) at most 96 rows name the same one
- gate_weights: float32 [4096, 8], P(('edp', 'ep')), may hold values from 0.05 to 0.5
- w_gate: bfloat16 [16, 2048, 768], P('ep'), may hold values from -0.125 to 0.125
- w_up: bfloat16 [16, 2048, 768], P('ep'), may hold values from -0.125 to 0.125
- w_down: bfloat16 [16, 768, 2048], P('ep'), may hold values from -0.21875 to 0.21875
- saved_inputs: bfloat16 [16, 512, 2048], P('ep', 'edp'), may hold values from -6 to 6
- saved_cotangent: bfloat16 [16, 512, 2048], P('ep', 'edp'), may hold values from -0.59765625 to 0.59765625
Outputs:
- mixed: bfloat16 [4096, 2048], P(('edp', 'ep'))
- grad_gate: float32 [16, 2048, 768], P('ep', 'edp')
- grad_up: float32 [16, 2048, 768], P('ep', 'edp')
- grad_down: float32 [16, 768, 2048], P('ep', 'edp')
The draws below stay inside these ranges and needn't reach their ends.
Inputs may be any that keep to these rules, and one draw needn't show every extreme that they name: `routes`: each token names 8 different experts. In each aligned block of 128 tokens (the tokens of one device) no expert is named more than 96 times, a bound that some block reaches in every draw.
All inputs are finite; a program needn't handle non-finite values.
Results may differ from the reference program's by a relative error of at most 0.006.
Values may be sent and summed in bfloat16 or wider, within the bound.
A program may use at most 128 MiB of HBM per device.

```python
import math
import jax
import jax.numpy as jnp
import numpy as np
from jax import lax

D = 2048
FF = 768
TOP = 8
TOK_DEV = 128
ROWS_BWD = 256
EXPERTS = 16
CAP = 96
TOKENS = 4096
BWD_ROWS = 512
N_EDP = 2


def levels(rng, dims, split, smallest, largest):
    gain, own = 1.0, jax.random.fold_in(rng, 6)
    for axis_at, blocks in split:
        steps = jnp.exp(jax.random.uniform(jax.random.fold_in(own, axis_at), (blocks,), jnp.float32, smallest / len(split), largest / len(split)))
        gain = gain * jnp.repeat(steps, dims[axis_at] // blocks).reshape([-1 if axis == axis_at else 1 for axis in range(len(dims))])
    return gain


def routed_block(stream_key, own, number, rows, number_of, top, reach, lean):
    order = jax.random.permutation(stream_key, number_of)
    packed, ordinary = portions_of(number_of, rows * top, reach, lean, True), portions_of(number_of, rows * top, reach, lean, False)
    places = jnp.arange(number_of)

    def named(tallies, offset_by):
        used = int((tallies > 0).sum())
        fixed = max(1, used // 4)
        shifted = fixed + (places - fixed + offset_by * (used - fixed)) % max(1, number_of - fixed)
        return jnp.zeros((number_of,), jnp.int32).at[order[jnp.where(places < fixed, places, shifted)]].set(jnp.asarray(tallies, jnp.int32))

    tallies = jnp.where(number % 4 == 0, named(packed, number // 4), named(ordinary, number - number // 4 - 1))
    mixed = jax.random.permutation(jax.random.fold_in(own, 3), number_of)
    source_of, receiver = mixed[0:number_of // 2 * 2:2], mixed[1:number_of // 2 * 2:2]
    margin = jnp.minimum(tallies[source_of] - 1, reach - tallies[receiver]) // 2
    margin = jnp.where((source_of == order[0]) | (receiver == order[0]) | (tallies[receiver] == 0), 0, jnp.maximum(margin, 0))
    shifted = jax.random.randint(jax.random.fold_in(own, 4), (number_of // 2,), 0, 1 << 20) % (margin + 1)
    tallies = tallies.at[source_of].add(-shifted).at[receiver].add(shifted)
    items = jnp.searchsorted(jnp.cumsum(tallies), jnp.arange(rows * top), side="right").astype(jnp.int32)
    listing = items.reshape(top, rows).T
    listing = listing[jax.random.permutation(jax.random.fold_in(own, 1), rows)]
    offset_by = jax.random.randint(jax.random.fold_in(own, 2), (rows, 1), 0, top)
    return jnp.take_along_axis(listing, (jnp.arange(top)[None, :] + offset_by) % top, axis=1)


def portions_of(amount, total, limit, slope, full):
    weights = [(1 << 20) // math.isqrt(rank ** slope) + 1 for rank in range(1, amount + 1)]
    largest = limit if full else min(limit, max(-(-total // amount), total * weights[0] // sum(weights)))
    least = 1 if total - largest >= amount - 1 else 0
    holding, surplus = [largest] + [least] * (amount - 1), total - largest - least * (amount - 1)
    while surplus > 0:
        movable = [i for i in range(1, amount) if holding[i] < largest] or [i for i in range(1, amount) if holding[i] < limit]
        mass, budget = sum([weights[i] for i in movable]), surplus
        for i in movable:
            addition = min(limit - holding[i], max(1, budget * weights[i] // mass), surplus)
            holding[i] = holding[i] + addition
            surplus = surplus - addition
    return np.array(holding)


def noise(own_key, extent, scale, most, shards=(), kind=jnp.bfloat16):
    drawn = jax.random.normal(own_key, extent, jnp.float32) * scale
    if len(shards) > 0:
        drawn = levels(own_key, extent, shards, -0.22, 0.18) * drawn
    return jnp.clip(drawn, min=-most, max=most).astype(kind)


def setup_inputs(seed: int = 0) -> dict:
    streams_of = jax.random.split(jax.random.key(seed), 9)
    tokens = noise(streams_of[0], (TOKENS, D), 1.0, 6.0, ((0, 32),))
    routes_keys = jax.random.split(jax.random.fold_in(streams_of[1], 1), TOKENS // TOK_DEV)
    routes_turns = jax.random.permutation(jax.random.fold_in(streams_of[1], 3), TOKENS // TOK_DEV)
    routes = jax.vmap(lambda own, number: routed_block(jax.random.fold_in(streams_of[1], 2), own, number, TOK_DEV, EXPERTS, TOP, CAP, 2))(routes_keys, routes_turns).reshape((TOKENS, TOP))
    gate_weights = jnp.clip(jnp.exp(math.log(0.5) - 2.3025851 * jax.random.uniform(streams_of[2], (TOKENS, TOP), jnp.float32) ** levels(streams_of[2], (TOKENS, TOP), ((0, 32),), -0.2, 0.2)), 0.05, 0.5)
    w_gate = noise(streams_of[3], (EXPERTS, D, FF), D ** -0.5, 0.125, ((0, 16),))
    w_up = noise(streams_of[4], (EXPERTS, D, FF), D ** -0.5, 0.125, ((0, 16),))
    w_down = noise(streams_of[5], (EXPERTS, FF, D), FF ** -0.5, 0.21875, ((0, 16),))
    saved_inputs = noise(streams_of[6], (EXPERTS, BWD_ROWS, D), 1.0, 6.0, ((0, 16), (1, 2)))
    saved_cotangent = noise(streams_of[7], (EXPERTS, BWD_ROWS, D), 0.1, 0.59765625, ((0, 16), (1, 2)))
    return {"tokens": tokens, "routes": routes, "gate_weights": gate_weights, "w_gate": w_gate, "w_up": w_up, "w_down": w_down, "saved_inputs": saved_inputs, "saved_cotangent": saved_cotangent}


def expert_mlp(row_data, w_gate, w_up, w_down):
    gate_pre = jnp.dot(row_data, w_gate, preferred_element_type=jnp.float32)
    up_pre = jnp.dot(row_data, w_up, preferred_element_type=jnp.float32)
    hidden = (jax.nn.silu(gate_pre) * up_pre).astype(jnp.bfloat16)
    return jnp.dot(hidden, w_down, preferred_element_type=jnp.float32).astype(jnp.bfloat16)


def expert_grads(inputs, cotangent, w_gate, w_up, w_down):
    gate_pre = jnp.dot(inputs, w_gate, preferred_element_type=jnp.float32)
    up_pre = jnp.dot(inputs, w_up, preferred_element_type=jnp.float32)
    activated = jax.nn.silu(gate_pre)
    hidden = (activated * up_pre).astype(jnp.bfloat16)
    d_hidden = jnp.dot(cotangent, w_down.T, preferred_element_type=jnp.float32)
    sigmoid_gate = jax.nn.sigmoid(gate_pre)
    d_gate = (d_hidden * up_pre * sigmoid_gate * (1.0 + gate_pre * (1.0 - sigmoid_gate))).astype(jnp.bfloat16)
    d_up = (d_hidden * activated).astype(jnp.bfloat16)
    return hidden, d_gate, d_up


def rounded(value):
    return lax.optimization_barrier(value.astype(jnp.bfloat16)).astype(jnp.float32)


def reference(tokens, routes, gate_weights, w_gate, w_up, w_down, saved_inputs, saved_cotangent):
    blocks = TOKENS // TOK_DEV
    route_blocks = routes.reshape(blocks, TOK_DEV * TOP)
    one_hot = (route_blocks[:, :, None] == jnp.arange(EXPERTS, dtype=jnp.int32)[None, None, :]).astype(jnp.int32)
    running = jnp.cumsum(one_hot, axis=1) - 1
    slot_index = jnp.sum(running * one_hot, axis=2)
    position = jnp.arange(blocks, dtype=jnp.int32)[:, None] * CAP + slot_index
    token_id = (jnp.arange(TOKENS * TOP, dtype=jnp.int32) // TOP).astype(jnp.int32)
    row_count = blocks * CAP
    row_table = jnp.full((EXPERTS, row_count), TOKENS, jnp.int32)
    row_table = row_table.at[route_blocks.reshape(-1), position.reshape(-1)].set(token_id)
    weight_table = jnp.zeros((EXPERTS, row_count), jnp.float32)
    weight_table = weight_table.at[route_blocks.reshape(-1), position.reshape(-1)].set(gate_weights.reshape(-1))
    padded = jnp.concatenate([tokens, jnp.zeros((1, D), tokens.dtype)], axis=0)

    def one_expert(accum_rows, expert_data):
        row_ids, weights, gate_mat, up_mat, down_mat = expert_data
        output = expert_mlp(padded[row_ids], gate_mat, up_mat, down_mat)
        accum_rows = accum_rows.at[row_ids].add(weights[:, None] * output.astype(jnp.float32))
        return accum_rows, None

    summed, unused = lax.scan(one_expert, jnp.zeros((TOKENS + 1, D), jnp.float32),
                              (row_table, weight_table, w_gate, w_up, w_down))
    mixed = summed[:TOKENS].astype(jnp.bfloat16)

    def expert_backward(expert_data):
        inputs_all, cotangent_all, gate_mat, up_mat, down_mat = expert_data
        grad_g = jnp.zeros((D, FF), jnp.float32)
        grad_u = jnp.zeros((D, FF), jnp.float32)
        grad_d = jnp.zeros((FF, D), jnp.float32)
        for replica in range(N_EDP):
            inputs = inputs_all[replica * ROWS_BWD:(replica + 1) * ROWS_BWD]
            cotangent = cotangent_all[replica * ROWS_BWD:(replica + 1) * ROWS_BWD]
            hidden, d_gate, d_up = expert_grads(inputs, cotangent, gate_mat, up_mat, down_mat)
            grad_g = grad_g + rounded(jnp.dot(inputs.T, d_gate, preferred_element_type=jnp.float32))
            grad_u = grad_u + rounded(jnp.dot(inputs.T, d_up, preferred_element_type=jnp.float32))
            grad_d = grad_d + rounded(jnp.dot(hidden.T, cotangent, preferred_element_type=jnp.float32))
        return grad_g, grad_u, grad_d

    grad_gate, grad_up, grad_down = lax.map(expert_backward, (saved_inputs, saved_cotangent, w_gate, w_up, w_down))
    return mixed, grad_gate, grad_up, grad_down
```

```python
import functools

import jax
import jax.numpy as jnp
from jax import lax
from jax.experimental import pallas as pl
from jax.experimental.pallas import tpu as pltpu
from jax.sharding import PartitionSpec as P

MESH = pl.DeviceIdType.MESH


def place():
    index = lax.axis_index("ep")
    return index, index // 4, (index // 2) % 2, index % 2


def gather_kernel(
    line, tok, tab, inp, cot, tok_o, tab_o, inp_o, cot_o,
    local, up_s, down_s, line_r, pair_s, pair_r, core_s, core_r, rep_s, rep_r,
):
    index, z, x, c = place()
    rep = lax.axis_index("edp")
    pair_dev = index + 2 - 4 * x
    core_dev = index + 1 - 2 * c

    def block(zz, xx, cc):
        return (zz * 2 + xx) * 2 + cc

    def copies(blk, own, target, send, recv, slot):
        out = []
        for k, (first, array) in enumerate(((tok, tok_o), (tab, tab_o))):
            out.append(
                pltpu.make_async_remote_copy(
                    src_ref=first if own else array.at[blk],
                    dst_ref=array.at[blk],
                    send_sem=send.at[slot, k],
                    recv_sem=recv.at[slot, k],
                    device_id={"ep": target},
                    device_id_type=MESH,
                )
            )
        return out

    def up(zz, own):
        return copies(block(zz, x, c), own, index + 4, up_s, line_r, zz)

    def down(zz, own):
        return copies(block(zz, x, c), own, index - 4, down_s, line_r, zz)

    def pair(zz, own, xx):
        return copies(block(zz, xx, c), own, pair_dev, pair_s, pair_r, zz)

    def core(zz, xx, own, cc):
        return copies(block(zz, xx, cc), own, core_dev, core_s, core_r, zz * 2 + xx)

    def start(items):
        for item in items:
            item.start()

    def landed(items):
        for item in items:
            item.wait_recv()

    def sent(items):
        for item in items:
            item.wait_send()

    def replica(k):
        other = 1 - rep
        source, target = ((inp, inp_o), (cot, cot_o))[k]
        return pltpu.make_async_remote_copy(
            src_ref=source,
            dst_ref=target.at[rep],
            send_sem=rep_s.at[k],
            recv_sem=rep_r.at[k],
            device_id={"edp": other},
            device_id_type=MESH,
        )

    keep = [
        pltpu.make_async_copy(tok, tok_o.at[index], local.at[0]),
        pltpu.make_async_copy(tab, tab_o.at[index], local.at[1]),
        pltpu.make_async_copy(inp, inp_o.at[rep], local.at[2]),
        pltpu.make_async_copy(cot, cot_o.at[rep], local.at[3]),
    ]

    @pl.when(z < line - 1)
    def _():
        start(up(z, True))

    @pl.when(z > 0)
    def _():
        start(down(z, True))

    start(pair(z, True, x))
    replica(0).start()
    replica(1).start()
    start(core(z, x, True, c))
    start(keep)

    def from_pair(zz):
        landed(pair(zz, False, 1 - x))
        start(core(zz, 1 - x, False, c))

    for d in range(1, line + 1):
        if d < line:

            @pl.when(z >= d)
            def _(d=d):
                landed(up(z - d, False))

                @pl.when(z < line - 1)
                def _():
                    start(up(z - d, False))

                start(pair(z - d, False, x))
                start(core(z - d, x, False, c))

            @pl.when(z + d < line)
            def _(d=d):
                landed(down(z + d, False))

                @pl.when(z > 0)
                def _():
                    start(down(z + d, False))

                start(pair(z + d, False, x))
                start(core(z + d, x, False, c))

        e = d - 1
        if e == 0:
            from_pair(z)
        else:

            @pl.when(z >= e)
            def _(e=e):
                from_pair(z - e)

            @pl.when(z + e < line)
            def _(e=e):
                from_pair(z + e)

    for zz in range(line):
        for xx in range(2):
            landed(core(zz, xx, False, 1 - c))
            sent(core(zz, xx, False, c))
        sent(pair(zz, False, x))

        @pl.when((z >= zz) & (z < line - 1))
        def _(zz=zz):
            sent(up(zz, False))

        @pl.when((z <= zz) & (z > 0))
        def _(zz=zz):
            sent(down(zz, False))

    for k in range(2):
        replica(k).wait()
    for item in keep:
        item.wait()


def gather(tokens, table, inputs, cotangent):
    size = lax.axis_size("ep")
    replicas = lax.axis_size("edp")
    line = size // 4
    dma = pltpu.SemaphoreType.DMA
    return pl.pallas_call(
        functools.partial(gather_kernel, line),
        out_shape=(
            jax.ShapeDtypeStruct((size,) + tokens.shape, tokens.dtype),
            jax.ShapeDtypeStruct((size,) + table.shape, table.dtype),
            jax.ShapeDtypeStruct((replicas,) + inputs.shape, inputs.dtype),
            jax.ShapeDtypeStruct((replicas,) + cotangent.shape, cotangent.dtype),
        ),
        in_specs=[pl.BlockSpec(memory_space=pltpu.VMEM)] * 4,
        out_specs=(pl.BlockSpec(memory_space=pl.ANY),) * 4,
        scratch_shapes=[
            dma((4,)),
            dma((line, 2)),
            dma((line, 2)),
            dma((line, 2)),
            dma((line, 2)),
            dma((line, 2)),
            dma((line * 2, 2)),
            dma((line * 2, 2)),
            dma((2,)),
            dma((2,)),
        ],
        compiler_params=pltpu.CompilerParams(has_side_effects=True),
        name="gather",
    )(tokens, table, inputs, cotangent)


def reduce_kernel(
    line, part, out, own, rc, sx, rx, ru, rd, su, sd, acc,
    local, core_s, core_r, pair_s, pair_r, up_s, up_r, down_s, down_r,
):
    index, z, x, c = place()
    pair_dev = index + 2 - 4 * x
    core_dev = index + 1 - 2 * c
    rows = out.shape[0]

    def remote(src, dst, send, recv, target, slot):
        return pltpu.make_async_remote_copy(
            src_ref=src, dst_ref=dst, send_sem=send.at[slot], recv_sem=recv.at[slot],
            device_id={"ep": target}, device_id_type=MESH,
        )

    def core(t, xx):
        slot = t * 2 + xx
        return remote(part.at[slot * 2 + 1 - c], rc.at[slot], core_s, core_r, core_dev, slot)

    def load(t, xx):
        slot = t * 2 + xx
        return pltpu.make_async_copy(part.at[slot * 2 + c], own.at[slot], local.at[slot])

    def pair(t):
        return remote(sx.at[t], rx.at[t], pair_s, pair_r, pair_dev, t)

    def up(t):
        return remote(su.at[t], ru.at[t], up_s, up_r, index + 4, t)

    def down(t):
        return remote(sd.at[t], rd.at[t], down_s, down_r, index - 4, t)

    def each_target(body):
        for d in range(line - 1, 0, -1):

            @pl.when(z + d < line)
            def _(d=d):
                body(z + d, 1)

            @pl.when(z >= d)
            def _(d=d):
                body(z - d, -1)

        body(z, 0)

    def slabs(step):
        def one(i, carry):
            step(pl.ds(pl.multiple_of(i * 16, 16), 16))
            return carry

        lax.fori_loop(0, rows // 16, one, 0)

    def base(t, xx):
        slot = t * 2 + xx
        load(t, xx).wait()
        core(t, xx).wait_recv()
        return slot

    def begin(xx):
        def body(t, side):
            core(t, xx).start()
            load(t, xx).start()

        return body

    each_target(begin(1 - x))
    each_target(begin(x))

    def cross(t, side):
        slot = base(t, 1 - x)

        def step(r):
            total = own[slot, r, :].astype(jnp.float32) + rc[slot, r, :].astype(jnp.float32)
            sx[t, r, :] = total.astype(jnp.bfloat16)

        slabs(step)
        pair(t).start()

    each_target(cross)

    def join(source, t):
        def step(r):
            acc[r, :] += source[t, r, :].astype(jnp.float32)

        slabs(step)

    def along(t, side):
        slot = base(t, x)
        pair(t).wait_recv()

        def step(r):
            total = own[slot, r, :].astype(jnp.float32) + rc[slot, r, :].astype(jnp.float32)
            acc[r, :] = total + rx[t, r, :].astype(jnp.float32)

        slabs(step)
        if side >= 0:

            @pl.when(z > 0)
            def _():
                up(t).wait_recv()
                join(ru, t)

        if side <= 0:

            @pl.when(z < line - 1)
            def _():
                down(t).wait_recv()
                join(rd, t)

        def finish(r):
            value = acc[r, :].astype(jnp.bfloat16)
            if side > 0:
                su[t, r, :] = value
            elif side < 0:
                sd[t, r, :] = value
            else:
                out[r, :] = value

        slabs(finish)
        if side > 0:
            up(t).start()
        elif side < 0:
            down(t).start()

    each_target(along)

    def drain(t, side):
        core(t, 0).wait_send()
        core(t, 1).wait_send()
        pair(t).wait_send()
        if side > 0:
            up(t).wait_send()
        elif side < 0:
            down(t).wait_send()

    each_target(drain)


def reduce(partial):
    size, rows, width = partial.shape
    line = size // 4
    dma = pltpu.SemaphoreType.DMA

    def slots(count):
        return pltpu.VMEM((count, rows, width), partial.dtype)

    return pl.pallas_call(
        functools.partial(reduce_kernel, line),
        out_shape=jax.ShapeDtypeStruct((rows, width), partial.dtype),
        in_specs=[pl.BlockSpec(memory_space=pl.ANY)],
        out_specs=pl.BlockSpec(memory_space=pltpu.VMEM),
        scratch_shapes=[slots(line * 2), slots(line * 2)]
        + [slots(line) for _ in range(6)]
        + [pltpu.VMEM((rows, width), jnp.float32)]
        + [dma((line * 2,))] * 3
        + [dma((line,))] * 6,
        compiler_params=pltpu.CompilerParams(has_side_effects=True, vmem_limit_bytes=40 << 20),
        name="reduce",
    )(partial)


def expert_mlp(row_data, w_gate, w_up, w_down):
    gate_pre = jnp.dot(row_data, w_gate, preferred_element_type=jnp.float32)
    up_pre = jnp.dot(row_data, w_up, preferred_element_type=jnp.float32)
    hidden = (jax.nn.silu(gate_pre) * up_pre).astype(jnp.bfloat16)
    return jnp.dot(hidden, w_down, preferred_element_type=jnp.float32)


def expert_grads(inputs, cotangent, w_gate, w_up, w_down):
    gate_pre = jnp.dot(inputs, w_gate, preferred_element_type=jnp.float32)
    up_pre = jnp.dot(inputs, w_up, preferred_element_type=jnp.float32)
    activated = jax.nn.silu(gate_pre)
    hidden = (activated * up_pre).astype(jnp.bfloat16)
    d_hidden = jnp.einsum("rd,fd->rf", cotangent, w_down, preferred_element_type=jnp.float32)
    sigmoid_gate = jax.nn.sigmoid(gate_pre)
    d_gate = (d_hidden * up_pre * sigmoid_gate * (1.0 + gate_pre * (1.0 - sigmoid_gate))).astype(
        jnp.bfloat16
    )
    d_up = (d_hidden * activated).astype(jnp.bfloat16)
    return (hidden, d_gate, d_up)


def shards(tokens, routes, gate_weights, w_gate, w_up, w_down, saved_inputs, saved_cotangent):
    experts = lax.axis_size("ep")
    tok_rows, width = tokens.shape
    gate_mat, up_mat, down_mat = (w_gate[0], w_up[0], w_down[0])
    hit = routes[None, :, :] == jnp.arange(experts, dtype=jnp.int32)[:, None, None]
    table = jnp.sum(jnp.where(hit, gate_weights[None], 0.0), axis=2)
    kernels = experts % 4 == 0 and experts <= 16 and lax.axis_size("edp") == 2
    if kernels:
        all_tokens, all_table, all_inputs, all_cotangent = gather(
            tokens, table, saved_inputs[0], saved_cotangent[0]
        )
        all_inputs = all_inputs.reshape(-1, width)
        all_cotangent = all_cotangent.reshape(-1, width)
        mine = lax.dynamic_index_in_dim(all_table, lax.axis_index("ep"), 1, keepdims=False)
    else:
        all_tokens = lax.all_gather(tokens, "ep", axis=0)
        mine = lax.all_to_all(table, "ep", split_axis=0, concat_axis=0, tiled=True)
        all_inputs = lax.all_gather(saved_inputs[0], "edp", axis=0, tiled=True)
        all_cotangent = lax.all_gather(saved_cotangent[0], "edp", axis=0, tiled=True)
    output = expert_mlp(all_tokens.reshape(-1, width), gate_mat, up_mat, down_mat)
    partial = (output * mine.reshape(-1, 1)).astype(jnp.bfloat16)
    if kernels:
        combined = reduce(partial.reshape(experts, tok_rows, width))
    else:
        combined = lax.psum_scatter(partial, "ep", scatter_dimension=0, tiled=True)

    replicas = lax.axis_size("edp")
    own_index = lax.axis_index("edp")
    half_width = width // replicas
    half_hidden = gate_mat.shape[1] // replicas
    hidden, d_gate, d_up = expert_grads(all_inputs, all_cotangent, gate_mat, up_mat, down_mat)
    in_cols = lax.dynamic_slice_in_dim(all_inputs, own_index * half_width, half_width, 1)
    hidden_cols = lax.dynamic_slice_in_dim(hidden, own_index * half_hidden, half_hidden, 1)
    grad_g = jnp.einsum("rd,rf->df", in_cols, d_gate, preferred_element_type=jnp.float32)
    grad_u = jnp.einsum("rd,rf->df", in_cols, d_up, preferred_element_type=jnp.float32)
    grad_d = jnp.einsum("rf,rd->fd", hidden_cols, all_cotangent, preferred_element_type=jnp.float32)
    return (combined, grad_g[None], grad_u[None], grad_d[None])


def solution(mesh):
    return jax.shard_map(
        shards,
        mesh=mesh,
        in_specs=(
            P(("edp", "ep"), None),
            P(("edp", "ep"), None),
            P(("edp", "ep"), None),
            P("ep", None, None),
            P("ep", None, None),
            P("ep", None, None),
            P("ep", "edp", None),
            P("ep", "edp", None),
        ),
        out_specs=(
            P(("edp", "ep"), None),
            P("ep", "edp", None),
            P("ep", "edp", None),
            P("ep", "edp", None),
        ),
        check_vma=False,
    )
```
